32 devices in a mesh: groups: 2 (over x), hist: 8 (over z, y), users: 2 (over core).
Axes of the slice: x: 2, y: 2, z: 4, core: 2. Of those that a mesh axis runs over, the one named last changes fastest.
Arguments:
- targets: bfloat16 [4, 512, 1024], P(('groups', 'users'), 'hist'), parts along dimension 0, may hold values from -6 to 6
- hist_keys: bfloat16 [2, 4, 12288, 1024], P(None, ('groups', 'users'), 'hist'), parts along dimension 1, may hold values from -6 to 6
- hist_values: bfloat16 [2, 4, 12288, 1024], P(None, ('groups', 'users'), 'hist'), parts along dimension 1, may hold values from -6 to 6
- lengths: int32 [4], P(('groups', 'users')), parts along dimension 0, may hold values from 3072 to 12288
- cuts: int32 [4, 512], P(('groups', 'users')), parts along dimension 0, may hold values from 1 to 12288
- w_query: bfloat16 [2, 1024, 1024], replicated, may hold values from -0.1875 to 0.1875
- w_gate: bfloat16 [2, 1024, 1024], replicated, may hold values from -0.1875 to 0.1875
- w_out: bfloat16 [2, 1024, 1024], replicated, may hold values from -0.1875 to 0.1875
- ln_gain: float32 [2, 1024], replicated, may hold values from 0.1 to 1.9
Outputs:
- refined: bfloat16 [4, 512, 1024], P(('groups', 'users'), 'hist'), parts along dimension 0
The draws below stay inside these ranges and needn't reach their ends.
There are 2 independent parts, one for each index of `groups`. The reference program is written for one: setup_inputs(seed, part) draws one part's arguments, and reference() takes and returns one part's arrays. A program takes and returns all parts, laid end to end along the dimension named above; an argument that names none is the same for every part. Nothing has to cross between parts.
All inputs are finite; a program needn't handle non-finite values.
Results may differ from the reference program's by a relative error of at most 0.012.
Values may be sent and summed in bfloat16 or wider, within the bound.
No kernel may reach another device: no remote copies, remote signals or barrier semaphores. Data moves between devices by JAX's collectives and lax.ppermute only.
A program may use at most 128 MiB of HBM per device.

```python
import math
import jax
import jax.numpy as jnp
from jax import lax

D = 1024
HEADS = 8
LAYERS = 2
TGT = 512
HIST = 12288
USERS = 2


def plant(drawn, stream_key, least, largest):
    spot = [jax.random.randint(jax.random.fold_in(stream_key, axis), (), 0, length) for axis, length in enumerate(drawn.shape)]
    main_axis = drawn.shape.index(max(drawn.shape))
    next_to = spot[:main_axis] + [(spot[main_axis] + 1) % drawn.shape[main_axis]] + spot[main_axis + 1:]
    return drawn.at[tuple(spot)].set(least).at[tuple(next_to)].set(largest)


def block_levels(key, dims, cuts, low, high):
    gain = 1.0
    for position, blocks in cuts:
        steps = jax.random.uniform(jax.random.fold_in(jax.random.fold_in(key, 6), position), (blocks,), jnp.float32, low / len(cuts), high / len(cuts))
        gain = gain * jnp.repeat(jnp.exp(steps), dims[position] // blocks).reshape((-1,) + (1,) * (len(dims) - 1 - position))
    return gain


def gaussian(rng, dims, scale, bound, shards=(), kind=jnp.bfloat16):
    drawn = scale * jax.random.normal(rng, dims, jnp.float32)
    if shards:
        drawn = drawn * block_levels(rng, dims, shards, -0.22, 0.18)
    return jnp.clip(drawn, -bound, bound).astype(kind)


def setup_inputs(seed: int = 0, part: int = 0) -> dict:
    splits = jax.random.split(jax.random.key(seed), 10)
    own_keys = jax.random.split(jax.random.fold_in(splits[9], part), 10)
    return {
        "targets": gaussian(own_keys[0], (USERS, TGT, D), 1.0, 6.0, ((0, 2), (1, 8))),
        "hist_keys": gaussian(own_keys[1], (LAYERS, USERS, HIST, D), 1.0, 6.0, ((1, 2), (2, 8))),
        "hist_values": gaussian(own_keys[2], (LAYERS, USERS, HIST, D), 1.0, 6.0, ((1, 2), (2, 8))),
        "lengths": jax.random.randint(own_keys[3], (USERS,), HIST // 4, HIST + 1).astype(jnp.int32),
        "cuts": plant(jax.random.randint(own_keys[4], (USERS, TGT), 1, HIST + 1), jax.random.fold_in(own_keys[4], 1), 1, HIST).astype(jnp.int32),
        "w_query": gaussian(splits[5], (LAYERS, D, D), D ** -0.5, 0.1875),
        "w_gate": gaussian(splits[6], (LAYERS, D, D), D ** -0.5, 0.1875),
        "w_out": gaussian(splits[7], (LAYERS, D, D), D ** -0.5, 0.1875),
        "ln_gain": jnp.clip(1.0 + 0.18 * jax.random.normal(splits[8], (LAYERS, D), jnp.float32), 0.1, 1.9),
    }


def attend(queries, key_slab, value_slab, limits):
    head_size = D // HEADS
    factor = 1.0 / math.sqrt(head_size)
    positions = jnp.arange(HIST, dtype=jnp.int32)
    visible = positions[None, :] < limits[:, None]
    query_heads = queries.reshape(TGT, HEADS, head_size).transpose(1, 0, 2)
    key_heads = key_slab.reshape(HIST, HEADS, head_size).transpose(1, 0, 2)
    value_heads = value_slab.reshape(HIST, HEADS, head_size).transpose(1, 0, 2)

    def one_head(operands):
        query_head, key_head, value_head = operands
        scores = jnp.dot(query_head, key_head.T, preferred_element_type=jnp.float32) * factor
        weights = jnp.where(visible, jax.nn.silu(scores), 0.0).astype(jnp.bfloat16)
        return jnp.dot(weights, value_head, preferred_element_type=jnp.float32)
    outputs = lax.map(one_head, (query_heads, key_heads, value_heads))
    return outputs.transpose(1, 0, 2).reshape(TGT, D)

def finish(hidden, summed, gating, out_weight, gain_row):
    centre = lax.optimization_barrier(jnp.mean(summed, axis=-1, keepdims=True))
    spread = lax.optimization_barrier(jnp.mean(jnp.square(summed - centre), axis=-1, keepdims=True))
    normed = ((summed - centre) * lax.rsqrt(spread + 1e-05) * gain_row * gating).astype(jnp.bfloat16)
    update = jnp.dot(normed, out_weight, preferred_element_type=jnp.float32)
    return (hidden.astype(jnp.float32) + update).astype(jnp.bfloat16)

def reference(targets, hist_keys, hist_values, lengths, cuts, w_query, w_gate, w_out, ln_gain):
    results = []
    for member in range(USERS):
        hidden = targets[member]
        limits = jnp.minimum(cuts[member], lengths[member])
        for layer_index in range(LAYERS):
            queries = jax.nn.silu(jnp.dot(hidden, w_query[layer_index], preferred_element_type=jnp.float32)).astype(jnp.bfloat16)
            gating = jax.nn.silu(jnp.dot(hidden, w_gate[layer_index], preferred_element_type=jnp.float32))
            summed = attend(queries, hist_keys[layer_index, member], hist_values[layer_index, member], limits)
            hidden = finish(hidden, summed, gating, w_out[layer_index], ln_gain[layer_index])
        results.append(hidden)
    return jnp.stack(results)
```

```python
import functools
import math

import jax
import jax.numpy as jnp
from jax import lax
from jax.experimental import pallas as pl
from jax.experimental.pallas import tpu as pltpu
from jax.sharding import PartitionSpec as P

HEADS = 8
CHUNKS = 2
ROW_TILE = 256
HIST_TILE = 512


def attend_kernel(half_factor, split, q_ref, lim_ref, k_ref, v_ref, keep_ref, send_ref):
    rows = q_ref.shape[0]
    hist_rows = k_ref.shape[2]
    tile_rows = math.gcd(ROW_TILE, split)
    tile_hist = math.gcd(HIST_TILE, hist_rows)
    lane = lax.broadcasted_iota(jnp.int32, (tile_rows, tile_hist), 1)
    for r in range(0, rows, tile_rows):
        q = q_ref[r : r + tile_rows, :]
        lim = lim_ref[r : r + tile_rows, :1]
        acc = None
        for j in range(0, hist_rows, tile_hist):
            k = k_ref[0, 0, j : j + tile_hist, :]
            v = v_ref[0, 0, j : j + tile_hist, :]
            s = lax.dot_general(q, k, (((1,), (1,)), ((), ())), preferred_element_type=jnp.float32)
            h = s * half_factor
            w = h * jnp.tanh(h) + h
            w = jnp.where(lane < lim - j, w, 0.0).astype(jnp.bfloat16)
            part = jnp.dot(w, v, preferred_element_type=jnp.float32)
            acc = part if acc is None else acc + part
        if r < split:
            keep_ref[r : r + tile_rows, :] = acc
        else:
            send_ref[r - split : r - split + tile_rows, :] = acc.astype(send_ref.dtype)


def attend(q, lim, keys, values, layer, first_head, split):
    rows, width = q.shape
    hist_rows = keys.shape[2]
    dim = keys.shape[3] // HEADS
    heads = width // dim
    slab = pl.BlockSpec((1, 1, hist_rows, dim), lambda h: (layer, 0, 0, first_head + h))
    return pl.pallas_call(
        functools.partial(attend_kernel, 0.5 / math.sqrt(dim), split),
        grid=(heads,),
        in_specs=[
            pl.BlockSpec((rows, dim), lambda h: (0, h)),
            pl.BlockSpec(lim.shape, lambda h: (0, 0)),
            slab,
            slab,
        ],
        out_specs=[
            pl.BlockSpec((split, dim), lambda h: (0, h)),
            pl.BlockSpec((rows - split, dim), lambda h: (0, h)),
        ],
        out_shape=[
            jax.ShapeDtypeStruct((split, width), jnp.float32),
            jax.ShapeDtypeStruct((rows - split, width), jnp.bfloat16),
        ],
        cost_estimate=pl.CostEstimate(
            flops=4 * rows * hist_rows * width,
            bytes_accessed=4 * hist_rows * width + 4 * rows * width,
            transcendentals=rows * hist_rows * heads,
        ),
        compiler_params=pltpu.CompilerParams(dimension_semantics=("arbitrary",)),
    )(q, lim, keys, values)


def finish(hidden, summed, gating, out_weight, gain_row):
    centre = jnp.mean(summed, axis=-1, keepdims=True)
    spread = jnp.mean(jnp.square(summed - centre), axis=-1, keepdims=True)
    normed = ((summed - centre) * lax.rsqrt(spread + 1e-05) * gain_row * gating).astype(
        jnp.bfloat16
    )
    update = jnp.dot(normed, out_weight, preferred_element_type=jnp.float32)
    return (hidden.astype(jnp.float32) + update).astype(jnp.bfloat16)


def per_device(size, targets, hist_keys, hist_values, lengths, cuts, w_query, w_gate, w_out, ln_gain):
    deep = 2 if size % 2 == 0 else 1
    long = size // deep
    me = lax.axis_index("hist")

    def shift_long(x, step):
        pairs = [
            (z * deep + y, (z + step) % long * deep + y) for z in range(long) for y in range(deep)
        ]
        return lax.ppermute(x, "hist", pairs)

    def swap_deep(x):
        pairs = [(z * deep + y, z * deep + (y ^ 1)) for z in range(long) for y in range(deep)]
        return lax.ppermute(x, "hist", pairs)

    hidden = targets[0]
    own_rows, width = hidden.shape
    hist_rows = hist_keys.shape[2]
    layers = hist_keys.shape[0]
    split = long * own_rows
    limits = (jnp.minimum(cuts[0], lengths[0]) - me * hist_rows).reshape(size, own_rows)
    ahead = jnp.arange(long)
    mine = (me // deep + ahead) % long * deep
    order = jnp.concatenate([mine + (me % deep ^ y) for y in range(deep)])
    limits = jnp.take(limits, order, axis=0).reshape(-1, 1)
    limits = jnp.broadcast_to(limits, (limits.shape[0], 128))
    part = width // CHUNKS

    for layer in range(layers):
        queries = jax.nn.silu(
            jnp.dot(hidden, w_query[layer], preferred_element_type=jnp.float32)
        ).astype(jnp.bfloat16)
        gating = jax.nn.silu(jnp.dot(hidden, w_gate[layer], preferred_element_type=jnp.float32))
        gathered = []
        for c in range(CHUNKS):
            own = queries[:, c * part : (c + 1) * part]
            blocks = jnp.concatenate([own] + [shift_long(own, -s) for s in range(1, long)])
            if deep > 1:
                blocks = jnp.concatenate([blocks, swap_deep(blocks)])
            gathered.append(blocks)
        sums = []
        for c in range(CHUNKS):
            keep, send = attend(
                gathered[c], limits, hist_keys, hist_values, layer, c * HEADS // CHUNKS, split
            )
            if deep > 1:
                keep = keep + swap_deep(send).astype(jnp.float32)
            total = keep[:own_rows]
            for s in range(1, long):
                block = keep[s * own_rows : (s + 1) * own_rows].astype(jnp.bfloat16)
                total = total + shift_long(block, s).astype(jnp.float32)
            sums.append(total)
        summed = jnp.concatenate(sums, axis=1)
        hidden = finish(hidden, summed, gating, w_out[layer], ln_gain[layer])
    return hidden[None]


def solution(mesh):
    return jax.shard_map(
        functools.partial(per_device, mesh.shape["hist"]),
        mesh=mesh,
        in_specs=(
            P(("groups", "users"), "hist", None),
            P(None, ("groups", "users"), "hist", None),
            P(None, ("groups", "users"), "hist", None),
            P(("groups", "users")),
            P(("groups", "users"), None),
            P(),
            P(),
            P(),
            P(),
        ),
        out_specs=P(("groups", "users"), "hist", None),
        check_vma=False,
    )
```

```python
import functools
import math

import jax
import jax.numpy as jnp
from jax import lax
from jax.experimental import pallas as pl
from jax.experimental.pallas import tpu as pltpu
from jax.sharding import PartitionSpec as P

HEADS = 8
CHUNKS = 2
ROW_TILE = 256
HIST_TILE = 512
STEP_HEADS = 2
LIMITS_COST = 20
ATTEND_VMEM = 16 * 2**20
FINISH_VMEM = 16 * 2**20


def limits_kernel(size, deep, step_long, hist_rows, length_ref, cuts_ref, *refs):
    outs, by_row = refs[:-1], refs[-1]
    me = lax.axis_index("hist")
    limit = jnp.minimum(cuts_ref[...], length_ref[0]) - me * hist_rows
    by_row[...] = jnp.broadcast_to(limit, (by_row.shape[1], limit.shape[1])).T
    own_rows = by_row.shape[0] // size
    z, y = me // deep, me % deep
    for across, out in enumerate(outs):
        for step in range(size // deep):
            owner = step_long(z, step) * deep + (y ^ across)
            rows = pl.ds(pl.multiple_of(owner * own_rows, own_rows), own_rows)
            out[step * own_rows : (step + 1) * own_rows, :] = by_row[rows, :]


def row_limits(size, deep, step_long, hist_rows, lengths, cuts):
    rows = cuts.shape[1]
    out = jax.ShapeDtypeStruct((rows // deep, 128), jnp.int32)
    return pl.pallas_call(
        functools.partial(limits_kernel, size, deep, step_long, hist_rows),
        in_specs=[
            pl.BlockSpec(memory_space=pltpu.SMEM),
            pl.BlockSpec(memory_space=pltpu.VMEM),
        ],
        out_shape=[out] * deep,
        scratch_shapes=[pltpu.VMEM((rows, 128), jnp.int32)],
        cost_estimate=pl.CostEstimate(
            flops=LIMITS_COST * 10**9, bytes_accessed=LIMITS_COST * 2 * 10**6, transcendentals=0
        ),
        compiler_params=pltpu.CompilerParams(vmem_limit_bytes=4 * 2**20),
    )(lengths, cuts)


def attend_kernel(dim, q_ref, lim_ref, k_ref, v_ref, out_ref):
    rows, width = q_ref.shape
    hist_rows = k_ref.shape[2]
    tile_rows = math.gcd(ROW_TILE, rows)
    tile_hist = math.gcd(HIST_TILE, hist_rows)
    lane = lax.broadcasted_iota(jnp.int32, (tile_rows, tile_hist), 1)
    for c in range(0, width, dim):
        head = slice(c, c + dim)
        for r in range(0, rows, tile_rows):
            q = q_ref[r : r + tile_rows, head]
            lim = lim_ref[r : r + tile_rows, :1]

            def score(j):
                k = k_ref[0, 0, j : j + tile_hist, head]
                return lax.dot_general(
                    q, k, (((1,), (1,)), ((), ())), preferred_element_type=jnp.float32
                )

            acc = None
            ahead = score(0)
            for j in range(0, hist_rows, tile_hist):
                h = ahead
                if j + tile_hist < hist_rows:
                    ahead = score(j + tile_hist)
                w = h * jnp.tanh(h) + h
                w = jnp.where(lane < lim - j, w, 0.0).astype(jnp.bfloat16)
                v = v_ref[0, 0, j : j + tile_hist, head]
                part = jnp.dot(w, v, preferred_element_type=jnp.float32)
                acc = part if acc is None else acc + part
            out_ref[r : r + tile_rows, head] = acc.astype(out_ref.dtype)


def attend(q, lim, keys, values, layer, first_head, dim, out_type):
    rows, width = q.shape
    hist_rows = keys.shape[2]
    step = STEP_HEADS * dim
    first = first_head // STEP_HEADS
    slab = pl.BlockSpec((1, 1, hist_rows, step), lambda h: (layer, 0, 0, first + h))
    return pl.pallas_call(
        functools.partial(attend_kernel, dim),
        grid=(width // step,),
        in_specs=[
            pl.BlockSpec((rows, step), lambda h: (0, h)),
            pl.BlockSpec(lim.shape, lambda h: (0, 0)),
            slab,
            slab,
        ],
        out_specs=pl.BlockSpec((rows, step), lambda h: (0, h)),
        out_shape=jax.ShapeDtypeStruct((rows, width), out_type),
        cost_estimate=pl.CostEstimate(
            flops=4 * rows * hist_rows * width,
            bytes_accessed=4 * hist_rows * width + 4 * rows * width,
            transcendentals=rows * hist_rows * width // dim,
        ),
        compiler_params=pltpu.CompilerParams(
            dimension_semantics=("arbitrary",), vmem_limit_bytes=ATTEND_VMEM
        ),
    )(q, lim, keys, values)


def finish_kernel(half_factor, layer, counts, hidden_ref, gate_ref, gain_ref, out_w_ref, query_w_ref, *refs):
    terms, outs = refs[: sum(counts)], refs[sum(counts) :]
    parts, first = [], 0
    for count in counts:
        total = terms[first][...].astype(jnp.float32)
        for term in terms[first + 1 : first + count]:
            total = total + term[...].astype(jnp.float32)
        parts.append(total)
        first += count
    summed = jnp.concatenate(parts, axis=1)
    centred = summed - jnp.mean(summed, axis=-1, keepdims=True)
    spread = jnp.mean(centred * centred, axis=-1, keepdims=True)
    normed = (centred * lax.rsqrt(spread + 1e-05) * gain_ref[...] * gate_ref[...]).astype(
        jnp.bfloat16
    )
    update = jnp.dot(normed, out_w_ref[layer], preferred_element_type=jnp.float32)
    hidden = (hidden_ref[...].astype(jnp.float32) + update).astype(jnp.bfloat16)
    outs[0][...] = hidden
    if len(outs) > 1:
        queries = jnp.dot(hidden, query_w_ref[layer + 1], preferred_element_type=jnp.float32)
        queries = (queries / (1.0 + jnp.exp(-queries)) * half_factor).astype(jnp.bfloat16)
        part = queries.shape[1] // (len(outs) - 1)
        for c, out in enumerate(outs[1:]):
            out[...] = queries[:, c * part : (c + 1) * part]


def finish(hidden, gating, gain, w_out, w_query, layer, terms, half_factor, last):
    rows, width = hidden.shape
    flat = [t for group in terms for t in group]
    outs = [jax.ShapeDtypeStruct((rows, width), jnp.bfloat16)]
    if not last:
        outs += [jax.ShapeDtypeStruct((rows, width // CHUNKS), jnp.bfloat16)] * CHUNKS
    return pl.pallas_call(
        functools.partial(finish_kernel, half_factor, layer, [len(group) for group in terms]),
        out_shape=outs,
        cost_estimate=pl.CostEstimate(
            flops=4 * rows * width * width,
            bytes_accessed=4 * width * width,
            transcendentals=rows * width,
        ),
        compiler_params=pltpu.CompilerParams(vmem_limit_bytes=FINISH_VMEM),
    )(hidden, gating, gain, w_out, w_query, *flat)


def per_device(size, targets, hist_keys, hist_values, lengths, cuts, w_query, w_gate, w_out, ln_gain):
    deep = 2 if size % 2 == 0 else 1
    long = size // deep
    paired = long & (long - 1) == 0

    def step_long(z, step):
        return z ^ step if paired else (z + step) % long

    def shift_long(x, step):
        pairs = [(z * deep + y, step_long(z, step) * deep + y) for z in range(long) for y in range(deep)]
        return lax.ppermute(x, "hist", pairs)

    def swap_deep(x):
        pairs = [(z * deep + y, z * deep + (y ^ 1)) for z in range(long) for y in range(deep)]
        return lax.ppermute(x, "hist", pairs)

    hidden = targets[0]
    own_rows, width = hidden.shape
    hist_rows = hist_keys.shape[2]
    layers = hist_keys.shape[0]
    part = width // CHUNKS
    dim = width // HEADS
    half_factor = 0.5 / math.sqrt(dim)
    lims = row_limits(size, deep, step_long, hist_rows, lengths, cuts)

    queries = []
    for c in range(CHUNKS):
        q = jax.nn.silu(
            jnp.dot(
                hidden,
                w_query[0, :, c * part : (c + 1) * part],
                preferred_element_type=jnp.float32,
            )
        )
        queries.append((q * half_factor).astype(jnp.bfloat16))

    for layer in range(layers):
        last = layer == layers - 1
        gating = jax.nn.silu(jnp.dot(hidden, w_gate[layer], preferred_element_type=jnp.float32))
        near, far = [], []
        for c in range(CHUNKS):
            q = queries[c]
            blocks = [q] + [
                shift_long(q, s if paired else -s) for s in range(1, long)
            ]
            near.append(jnp.concatenate(blocks))
            if deep > 1:
                far.append(swap_deep(near[c]))
        terms = []
        before = None
        for c in range(CHUNKS):
            where = (hist_keys, hist_values, layer, c * HEADS // CHUNKS, dim)
            query = near[c]
            if before is not None:
                query, before = lax.optimization_barrier((query, before))
            keep = attend(query, lims[0], *where, jnp.float32)
            before = keep
            if deep > 1:
                query, before = lax.optimization_barrier((far[c], before))
                send = attend(query, lims[1], *where, jnp.bfloat16)
                before = send
                keep = keep + swap_deep(send).astype(jnp.float32)
            group = [keep[:own_rows]]
            for s in range(1, long):
                block = keep[s * own_rows : (s + 1) * own_rows].astype(jnp.bfloat16)
                group.append(shift_long(block, s))
            terms.append(group)
        gain = ln_gain[layer : layer + 1]
        hidden, *queries = finish(
            hidden, gating, gain, w_out, w_query, layer, terms, half_factor, last
        )
    return hidden[None]


def solution(mesh):
    return jax.shard_map(
        functools.partial(per_device, mesh.shape["hist"]),
        mesh=mesh,
        in_specs=(
            P(("groups", "users"), "hist", None),
            P(None, ("groups", "users"), "hist", None),
            P(None, ("groups", "users"), "hist", None),
            P(("groups", "users")),
            P(("groups", "users"), None),
            P(),
            P(),
            P(),
            P(),
        ),
        out_specs=P(("groups", "users"), "hist", None),
        check_vma=False,
    )
```

```python
import functools
import math

import jax
import jax.numpy as jnp
from jax import lax
from jax.experimental import pallas as pl
from jax.experimental.pallas import tpu as pltpu
from jax.sharding import PartitionSpec as P

HEADS = 8
CHUNKS = 2
ROW_TILE = 256
HIST_TILE = 512
STEP_HEADS = 4
LIMITS_COST = 20
ATTEND_VMEM = 16 * 2**20
FINISH_VMEM = 16 * 2**20


def limits_kernel(size, deep, step_long, hist_rows, length_ref, cuts_ref, *refs):
    outs, by_row = refs[:-1], refs[-1]
    me = lax.axis_index("hist")
    limit = jnp.minimum(cuts_ref[...], length_ref[0]) - me * hist_rows
    by_row[...] = jnp.broadcast_to(limit, (by_row.shape[1], limit.shape[1])).T
    own_rows = by_row.shape[0] // size
    z, y = me // deep, me % deep
    for across, out in enumerate(outs):
        for step in range(size // deep):
            owner = step_long(z, step) * deep + (y ^ across)
            rows = pl.ds(pl.multiple_of(owner * own_rows, own_rows), own_rows)
            out[step * own_rows : (step + 1) * own_rows, :] = by_row[rows, :]


def row_limits(size, deep, step_long, hist_rows, lengths, cuts):
    rows = cuts.shape[1]
    out = jax.ShapeDtypeStruct((rows // deep, 128), jnp.int32)
    return pl.pallas_call(
        functools.partial(limits_kernel, size, deep, step_long, hist_rows),
        in_specs=[
            pl.BlockSpec(memory_space=pltpu.SMEM),
            pl.BlockSpec(memory_space=pltpu.VMEM),
        ],
        out_shape=[out] * deep,
        scratch_shapes=[pltpu.VMEM((rows, 128), jnp.int32)],
        cost_estimate=pl.CostEstimate(
            flops=LIMITS_COST * 10**9, bytes_accessed=LIMITS_COST * 2 * 10**6, transcendentals=0
        ),
        compiler_params=pltpu.CompilerParams(vmem_limit_bytes=4 * 2**20),
    )(lengths, cuts)


def attend_kernel(dim, q_ref, lim_ref, k_ref, v_ref, out_ref):
    rows, width = q_ref.shape
    hist_rows = k_ref.shape[2]
    tile_rows = math.gcd(ROW_TILE, rows)
    tile_hist = math.gcd(HIST_TILE, hist_rows)
    lane = lax.broadcasted_iota(jnp.int32, (tile_rows, tile_hist), 1)
    for c in range(0, width, dim):
        head = slice(c, c + dim)
        for r in range(0, rows, tile_rows):
            q = q_ref[r : r + tile_rows, head]
            lim = lim_ref[r : r + tile_rows, :]
            lim = jnp.concatenate([lim] * (tile_hist // lim.shape[1]), axis=1)

            def score(j):
                k = k_ref[0, 0, j : j + tile_hist, head]
                return lax.dot_general(
                    q, k, (((1,), (1,)), ((), ())), preferred_element_type=jnp.float32
                )

            acc = None
            ahead = score(0)
            for j in range(0, hist_rows, tile_hist):
                h = ahead
                if j + tile_hist < hist_rows:
                    ahead = score(j + tile_hist)
                w = h * jnp.tanh(h) + h
                w = jnp.where(lane < lim - j, w, 0.0).astype(jnp.bfloat16)
                v = v_ref[0, 0, j : j + tile_hist, head]
                part = jnp.dot(w, v, preferred_element_type=jnp.float32)
                acc = part if acc is None else acc + part
            out_ref[r : r + tile_rows, head] = acc.astype(out_ref.dtype)


def attend(q, lim, keys, values, layer, first_head, dim, out_type):
    rows, width = q.shape
    hist_rows = keys.shape[2]
    step = STEP_HEADS * dim
    first = first_head // STEP_HEADS
    slab = pl.BlockSpec((1, 1, hist_rows, step), lambda h: (layer, 0, 0, first + h))
    return pl.pallas_call(
        functools.partial(attend_kernel, dim),
        grid=(width // step,),
        in_specs=[
            pl.BlockSpec((rows, step), lambda h: (0, h)),
            pl.BlockSpec(lim.shape, lambda h: (0, 0)),
            slab,
            slab,
        ],
        out_specs=pl.BlockSpec((rows, step), lambda h: (0, h)),
        out_shape=jax.ShapeDtypeStruct((rows, width), out_type),
        cost_estimate=pl.CostEstimate(
            flops=4 * rows * hist_rows * width,
            bytes_accessed=4 * hist_rows * width + 4 * rows * width,
            transcendentals=rows * hist_rows * width // dim,
        ),
        compiler_params=pltpu.CompilerParams(
            dimension_semantics=("arbitrary",), vmem_limit_bytes=ATTEND_VMEM
        ),
    )(q, lim, keys, values)


def finish_kernel(half_factor, layer, counts, hidden_ref, gate_ref, gain_ref, out_w_ref, query_w_ref, *refs):
    terms, outs = refs[: sum(counts)], refs[sum(counts) :]
    parts, first = [], 0
    for count in counts:
        total = terms[first][...].astype(jnp.float32)
        for term in terms[first + 1 : first + count]:
            total = total + term[...].astype(jnp.float32)
        parts.append(total)
        first += count
    summed = jnp.concatenate(parts, axis=1)
    centred = summed - jnp.mean(summed, axis=-1, keepdims=True)
    spread = jnp.mean(centred * centred, axis=-1, keepdims=True)
    normed = (centred * lax.rsqrt(spread + 1e-05) * gain_ref[...] * gate_ref[...]).astype(
        jnp.bfloat16
    )
    update = jnp.dot(normed, out_w_ref[layer], preferred_element_type=jnp.float32)
    hidden = (hidden_ref[...].astype(jnp.float32) + update).astype(jnp.bfloat16)
    outs[0][...] = hidden
    if len(outs) > 1:
        queries = jnp.dot(hidden, query_w_ref[layer + 1], preferred_element_type=jnp.float32)
        queries = (queries / (1.0 + jnp.exp(-queries)) * half_factor).astype(jnp.bfloat16)
        part = queries.shape[1] // (len(outs) - 1)
        for c, out in enumerate(outs[1:]):
            out[...] = queries[:, c * part : (c + 1) * part]


def finish(hidden, gating, gain, w_out, w_query, layer, terms, half_factor, last):
    rows, width = hidden.shape
    flat = [t for group in terms for t in group]
    outs = [jax.ShapeDtypeStruct((rows, width), jnp.bfloat16)]
    if not last:
        outs += [jax.ShapeDtypeStruct((rows, width // CHUNKS), jnp.bfloat16)] * CHUNKS
    return pl.pallas_call(
        functools.partial(finish_kernel, half_factor, layer, [len(group) for group in terms]),
        out_shape=outs,
        cost_estimate=pl.CostEstimate(
            flops=4 * rows * width * width,
            bytes_accessed=4 * width * width,
            transcendentals=rows * width,
        ),
        compiler_params=pltpu.CompilerParams(vmem_limit_bytes=FINISH_VMEM),
    )(hidden, gating, gain, w_out, w_query, *flat)


def per_device(size, targets, hist_keys, hist_values, lengths, cuts, w_query, w_gate, w_out, ln_gain):
    deep = 2 if size % 2 == 0 else 1
    long = size // deep
    paired = long & (long - 1) == 0

    def step_long(z, step):
        return z ^ step if paired else (z + step) % long

    def shift_long(x, step):
        pairs = [(z * deep + y, step_long(z, step) * deep + y) for z in range(long) for y in range(deep)]
        return lax.ppermute(x, "hist", pairs)

    def swap_deep(x):
        pairs = [(z * deep + y, z * deep + (y ^ 1)) for z in range(long) for y in range(deep)]
        return lax.ppermute(x, "hist", pairs)

    hidden = targets[0]
    own_rows, width = hidden.shape
    hist_rows = hist_keys.shape[2]
    layers = hist_keys.shape[0]
    part = width // CHUNKS
    dim = width // HEADS
    half_factor = 0.5 / math.sqrt(dim)
    lims = row_limits(size, deep, step_long, hist_rows, lengths, cuts)

    queries = []
    for c in range(CHUNKS):
        q = jax.nn.silu(
            jnp.dot(
                hidden,
                w_query[0, :, c * part : (c + 1) * part],
                preferred_element_type=jnp.float32,
            )
        )
        queries.append((q * half_factor).astype(jnp.bfloat16))

    for layer in range(layers):
        last = layer == layers - 1
        gating = jax.nn.silu(jnp.dot(hidden, w_gate[layer], preferred_element_type=jnp.float32))
        near, far = [], []
        for c in range(CHUNKS):
            q = queries[c]
            blocks = [q]
            for s in range(1, long):
                blocks.append(shift_long(q, s if paired else -s))
            near.append(jnp.concatenate(blocks))
            if deep > 1:
                far.append(swap_deep(near[c]))
        terms = []
        before = None
        for c in range(CHUNKS):
            where = (hist_keys, hist_values, layer, c * HEADS // CHUNKS, dim)
            query = near[c]
            if before is not None:
                query, before = lax.optimization_barrier((query, before))
            keep = attend(query, lims[0], *where, jnp.float32)
            before = keep
            if deep > 1:
                query, before = lax.optimization_barrier((far[c], before))
                send = attend(query, lims[1], *where, jnp.bfloat16)
                before = send
                keep = keep + swap_deep(send).astype(jnp.float32)
            group = [keep[:own_rows]]
            for s in range(1, long):
                block = keep[s * own_rows : (s + 1) * own_rows].astype(jnp.bfloat16)
                group.append(shift_long(block, s))
            terms.append(group)
        gain = ln_gain[layer : layer + 1]
        hidden, *queries = finish(
            hidden, gating, gain, w_out, w_query, layer, terms, half_factor, last
        )
    return hidden[None]


def solution(mesh):
    return jax.shard_map(
        functools.partial(per_device, mesh.shape["hist"]),
        mesh=mesh,
        in_specs=(
            P(("groups", "users"), "hist", None),
            P(None, ("groups", "users"), "hist", None),
            P(None, ("groups", "users"), "hist", None),
            P(("groups", "users")),
            P(("groups", "users"), None),
            P(),
            P(),
            P(),
            P(),
        ),
        out_specs=P(("groups", "users"), "hist", None),
        check_vma=False,
    )
```
